8 devices in a mesh: frag: 1 (over z), dev: 8 (over y, x, core).
Axes of the slice: x: 2, y: 2, z: 1, core: 2. Of those that a mesh axis runs over, the one named last changes fastest.
Arguments:
- a_ints: bfloat16 [144, 144, 144, 144], P(('frag', 'dev'))
- c_occ: bfloat16 [144, 24], P('frag')
- c_vir: bfloat16 [144, 120], P('frag')
- eps_occ: float32 [24], P('frag')
- eps_vir: float32 [120], P('frag')
Outputs:
- output: float32 [24, 24], P('frag', 'dev')
All inputs are finite; a program needn't handle non-finite values.
Results may differ from the reference program's by a relative error of at most 0.001.
Values are sent between devices in bfloat16 or wider.
A program may use at most 1 GiB of HBM per device.

```python
import jax
import jax.numpy as jnp
from jax import lax

PAD_BASIS = 144
NUM_OCC = 24
NUM_VIRT = 120


def setup_inputs(seed: int = 0, part: int = 0) -> dict:
    key_base = jax.random.fold_in(jax.random.key(seed), part)
    key_ints, key_occ, key_vir, key_eocc, key_evir = jax.random.split(key_base, 5)

    def draw_row(row_idx):
        raw_row = jax.random.normal(jax.random.fold_in(key_ints, row_idx), (PAD_BASIS, PAD_BASIS, PAD_BASIS), jnp.float32)
        mixed_row = (raw_row + 0.5 * jnp.transpose(raw_row, (2, 1, 0))) * (1.25 ** -0.5)
        return mixed_row.astype(jnp.bfloat16)

    a_ints = lax.map(draw_row, jnp.arange(PAD_BASIS))
    c_occ = (jax.random.normal(key_occ, (PAD_BASIS, NUM_OCC), jnp.float32) * PAD_BASIS ** -0.5).astype(jnp.bfloat16)
    c_vir = (jax.random.normal(key_vir, (PAD_BASIS, NUM_VIRT), jnp.float32) * (PAD_BASIS * NUM_VIRT) ** -0.5).astype(jnp.bfloat16)
    eps_occ = jax.random.uniform(key_eocc, (NUM_OCC,), jnp.float32, -1.5, -0.5)
    eps_vir = jax.random.uniform(key_evir, (NUM_VIRT,), jnp.float32, 0.3, 2.0)
    return {"a_ints": a_ints, "c_occ": c_occ, "c_vir": c_vir, "eps_occ": eps_occ, "eps_vir": eps_vir}


def reference(a_ints, c_occ, c_vir, eps_occ, eps_vir):
    occ_32 = c_occ.astype(jnp.float32)
    vir_32 = c_vir.astype(jnp.float32)

    def first_half(a_row):
        t_one = jnp.einsum("qrs,rj->qsj", a_row.astype(jnp.float32), occ_32).astype(jnp.bfloat16)
        return jnp.einsum("qsj,sb->qjb", t_one.astype(jnp.float32), vir_32).astype(jnp.bfloat16)

    half_mo = lax.map(first_half, a_ints)
    g_mat = jnp.einsum("pqjb,qa->pjba", half_mo.astype(jnp.float32), vir_32).astype(jnp.bfloat16)
    v_mo = jnp.einsum("pjba,pi->jbai", g_mat.astype(jnp.float32), occ_32)
    v_swap = jnp.swapaxes(v_mo, 1, 2)
    denominator = (eps_occ[:, None, None, None] + eps_occ[None, None, None, :]
                   - eps_vir[None, :, None, None] - eps_vir[None, None, :, None])
    pair_ji = jnp.sum(v_mo * (2.0 * v_mo - v_swap) / denominator, axis=(1, 2))
    return pair_ji.T
```

```python
import functools

import jax
import jax.numpy as jnp
from jax import lax
from jax.experimental import pallas as pl
from jax.experimental.pallas import tpu as pltpu
from jax.sharding import PartitionSpec as P

MESH = pl.DeviceIdType.MESH
F32, BF16 = jnp.float32, jnp.bfloat16
NT = (((1,), (1,)), ((), ()))
LANES = 128
TILE = 16
QB = 16
SLOTS = 5


def iota(shape, dim):
    return lax.broadcasted_iota(jnp.int32, shape, dim)


def eye(n):
    return (iota((n, n), 0) == iota((n, n), 1)).astype(BF16)


def kernel(ndev, a_ref, co_ref, cv_ref, eo_ref, ev_ref, e_ref,
           abuf, t_scr, h_scr, g_scr, recv, v_scr, kron, cot, cvt, cvp, evrow, es,
           a_sem, send_sem, recv_sem):
    rows_p, n = a_ref.shape[0], a_ref.shape[1]
    o, v = co_ref.shape[1], cv_ref.shape[1]
    od = o // ndev
    pts = od * v
    nqb = n // QB
    nblk = rows_p * nqb
    me = lax.axis_index("dev")

    def partner(k):
        parts = [((me // s) % 2 + (k // s) % 2) % 2 * s for s in (4, 2, 1)]
        return parts[0] + parts[1] + parts[2]

    def fetch(blk):
        return pltpu.make_async_copy(
            a_ref.at[blk // nqb, pl.ds(blk % nqb * QB, QB)], abuf.at[blk % SLOTS], a_sem.at[blk % SLOTS])

    for s in range(SLOTS):
        fetch(s).start()

    barrier = pltpu.get_barrier_semaphore()
    for k in range(1, ndev):
        pl.semaphore_signal(barrier, inc=1, device_id={"dev": partner(k)}, device_id_type=MESH)

    cot[...] = lax.dot_general(eye(o), co_ref[...], NT, preferred_element_type=F32).astype(BF16)
    cvt[...] = lax.dot_general(eye(v), cv_ref[...], NT, preferred_element_type=F32).astype(BF16)
    cvp[...] = jnp.zeros_like(cvp)
    cvp[:, :v] = cv_ref[...]
    evrow[...] = jnp.ones_like(evrow)
    evrow[:, :v] = ev_ref[...]

    pl.semaphore_wait(barrier, ndev - 1)

    def send(k, p):
        return pltpu.make_async_remote_copy(
            src_ref=g_scr.at[p, partner(k)], dst_ref=recv.at[k - 1, p],
            send_sem=send_sem.at[k - 1, p], recv_sem=recv_sem.at[k - 1, p],
            device_id={"dev": partner(k)}, device_id_type=MESH)

    def row(p, _):
        def block(qb, _):
            blk = p * nqb + qb
            fetch(blk).wait()
            slot = blk % SLOTS
            for q in range(0, QB, 2):
                t = [jnp.dot(cot[...], abuf[slot, q + h], preferred_element_type=F32) for h in range(2)]
                t_scr[q * o:(q + 2) * o, :] = jnp.concatenate(t, 0).astype(BF16)
            h_scr[pl.ds(qb * QB * o, QB * o), :] = jnp.dot(t_scr[...], cvp[...], preferred_element_type=F32)

            @pl.when(blk + SLOTS < nblk)
            def _():
                fetch(blk + SLOTS).start()
            return 0

        lax.fori_loop(0, nqb, block, 0)
        for j in range(0, o, 2):
            h = jnp.concatenate([h_scr[pl.ds(j + x, n, stride=o), :] for x in range(2)], 1).astype(BF16)
            g = jnp.dot(cvt[...], h, preferred_element_type=F32).astype(BF16)
            for x in range(2):
                d, r = divmod(j + x, od)
                g_scr[p, d, r * v:(r + 1) * v, :] = g[:, x * LANES:(x + 1) * LANES]
        for k in (6, 7, 2, 3, 4, 5, 1):
            send(k, p).start()
        return 0

    lax.fori_loop(0, rows_p, row, 0)

    wide = 2 * ndev * TILE
    spread = (iota((o * TILE, o), 0) // TILE == iota((o * TILE, o), 1)).astype(BF16)
    cor = jnp.dot(spread, cot[...], preferred_element_type=F32).astype(BF16)
    col = iota((n, wide), 1) // TILE
    k = col // 2
    dev = ((me // 4 + k // 4) % 2) * 4 + ((me // 2 + k // 2) % 2) * 2 + (me + k) % 2
    src = dev * rows_p + col % 2
    keep = iota((o * TILE, wide), 0) % TILE == iota((o * TILE, wide), 1) % TILE
    for g in range(rows_p // 2):
        sel = (iota((n, wide), 0) == src + 2 * g).astype(BF16)
        m = jnp.dot(cor, sel, preferred_element_type=F32)
        kron[g] = jnp.where(keep, m, 0.0).astype(BF16)

    v_scr[...] = jnp.zeros_like(v_scr)

    def group(g, _):
        for s in range(1, ndev):
            for x in range(2):
                send(s, 2 * g + x).wait_recv()

        def rhs(r0):
            tiles = [g_scr[2 * g + x, me, pl.ds(r0, TILE), :] for x in range(2)]
            tiles += [recv[s, 2 * g + x, pl.ds(r0, TILE), :] for s in range(ndev - 1) for x in range(2)]
            return jnp.concatenate(tiles, 0)

        def pair(t, _):
            r0 = pl.multiple_of(t * 2 * TILE, 2 * TILE)
            out = jnp.dot(kron[g], jnp.concatenate([rhs(r0), rhs(r0 + TILE)], 1), preferred_element_type=F32)
            out = out.reshape(o, TILE, 2 * LANES)
            for x in range(2):
                v_scr[:, pl.ds(r0 + x * TILE, TILE), :] += out[:, :, x * LANES:(x + 1) * LANES]
            return 0

        full = pts // (2 * TILE)
        lax.fori_loop(0, full, pair, 0)
        rest = pts - full * 2 * TILE
        out = jnp.dot(kron[g], rhs(pts - TILE), preferred_element_type=F32).reshape(o, TILE, LANES)
        v_scr[:, pts - rest:pts, :] += out[:, TILE - rest:, :]
        return 0

    lax.fori_loop(0, rows_p // 2, group, 0)

    evb = jnp.broadcast_to(evrow[...], (LANES, LANES))
    evsum = (evb + evb.T)[:v]

    def energies(i, _):
        for j in range(od):
            x = v_scr[i, j * v:j * v + LANES, :]
            xt = x.T[:v]
            x = x[:v]
            e = x * (2.0 * x - xt) / (eo_ref[me * od + j] + eo_ref[i] - evsum)
            es[j, i] = jnp.sum(e.reshape(v // 8, 8, LANES), 0)
        return 0

    lax.fori_loop(0, o, energies, 0)
    for j in range(od):
        e_ref[:, j:j + 1] = jnp.sum(jnp.sum(es[j], 1), 1, keepdims=True)

    def drain(p, _):
        for s in range(1, ndev):
            send(s, p).wait_send()
        return 0

    lax.fori_loop(0, rows_p, drain, 0)


def solution(mesh):
    ndev = mesh.shape["dev"]

    def per_device(a_ints, c_occ, c_vir, eps_occ, eps_vir):
        rows_p, n = a_ints.shape[:2]
        o, v = c_occ.shape[1], c_vir.shape[1]
        od = o // ndev
        pts = od * v
        vm = pl.BlockSpec(memory_space=pltpu.VMEM)
        return pl.pallas_call(
            functools.partial(kernel, ndev),
            out_shape=jax.ShapeDtypeStruct((o, od), F32),
            in_specs=[pl.BlockSpec(memory_space=pl.ANY), vm, vm, pl.BlockSpec(memory_space=pltpu.SMEM), vm],
            out_specs=vm,
            scratch_shapes=[
                pltpu.VMEM((SLOTS, QB, n, n), BF16),
                pltpu.VMEM((QB * o, n), BF16),
                pltpu.VMEM((n * o, LANES), F32),
                pltpu.VMEM((rows_p, ndev, pts, LANES), BF16),
                pltpu.VMEM((ndev - 1, rows_p, pts, LANES), BF16),
                pltpu.VMEM((o, pts + 8, LANES), F32),
                pltpu.VMEM((rows_p // 2, o * TILE, 2 * ndev * TILE), BF16),
                pltpu.VMEM((o, n), BF16),
                pltpu.VMEM((v, n), BF16),
                pltpu.VMEM((n, LANES), BF16),
                pltpu.VMEM((1, LANES), F32),
                pltpu.VMEM((od, o, 8, LANES), F32),
                pltpu.SemaphoreType.DMA((SLOTS,)),
                pltpu.SemaphoreType.DMA((ndev - 1, rows_p)),
                pltpu.SemaphoreType.DMA((ndev - 1, rows_p)),
            ],
            compiler_params=pltpu.CompilerParams(
                collective_id=0, has_side_effects=True, vmem_limit_bytes=60 * 2**20),
        )(a_ints, c_occ, c_vir, eps_occ, eps_vir.reshape(1, v))

    return jax.shard_map(
        per_device,
        mesh=mesh,
        in_specs=(P(("frag", "dev")), P("frag"), P("frag"), P("frag"), P("frag")),
        out_specs=P("frag", "dev"),
        check_vma=False,
    )
```

```python
import functools

import jax
import jax.numpy as jnp
from jax import lax
from jax.experimental import pallas as pl
from jax.experimental.pallas import tpu as pltpu
from jax.sharding import PartitionSpec as P

MESH = pl.DeviceIdType.MESH
F32, BF16 = jnp.float32, jnp.bfloat16
NT = (((1,), (1,)), ((), ()))
LANES = 128
TILE = 16
QB = 16
CHUNKS = 3
IC = 4
CUT = 176
PG = 4


def iota(shape, dim):
    return lax.broadcasted_iota(jnp.int32, shape, dim)


def eye(n):
    return (iota((n, n), 0) == iota((n, n), 1)).astype(BF16)


def kernel(ndev, a_ref, co_ref, cv_ref, eo_ref, ev_ref, e_ref,
           abuf, t_scr, h_scr, g_scr, recv_a, recv_b, v_own, v_rel, v_in, kron, kron_last, cot, cvt, cvp, evrow, es,
           a_sem, send_sem, recv_sem, vsend_sem, vrecv_sem):
    rows_p, n = a_ref.shape[0], a_ref.shape[1]
    o, v = co_ref.shape[1], cv_ref.shape[1]
    od = o // ndev
    pts = od * v
    nqb = n // QB
    me = lax.axis_index("dev")
    recv = (recv_a, recv_b)
    cut = recv_a.shape[3]
    base = (0, cut)
    size = (cut, pts - cut)
    first = (2, 4)
    second = (4, 2)

    def partner(k):
        parts = [((me // s) % 2 + (k // s) % 2) % 2 * s for s in (4, 2, 1)]
        return parts[0] + parts[1] + parts[2]

    def slots(h):
        return (0, 1, first[h], first[h] + 1)

    def fetch(p, x):
        return pltpu.make_async_copy(a_ref.at[p, pl.ds(x * QB, QB)], abuf.at[x], a_sem.at[x])

    for x in range(nqb):
        fetch(0, x).start()

    barrier = pltpu.get_barrier_semaphore()
    for k in range(1, 6):
        pl.semaphore_signal(barrier, inc=1, device_id={"dev": partner(k)}, device_id_type=MESH)

    cot[...] = lax.dot_general(eye(o), co_ref[...], NT, preferred_element_type=F32).astype(BF16)
    cvt[...] = lax.dot_general(eye(v), cv_ref[...], NT, preferred_element_type=F32).astype(BF16)
    cvp[...] = jnp.zeros_like(cvp)
    cvp[:, :v] = cv_ref[...]
    evrow[...] = jnp.ones_like(evrow)
    evrow[:, :v] = ev_ref[...]

    pl.semaphore_wait(barrier, 5)

    def send(h, s, t, p):
        k = slots(h)[s]
        return pltpu.make_async_remote_copy(
            src_ref=g_scr.at[p, partner(k ^ (t * second[h])), pl.ds(base[h], size[h])],
            dst_ref=recv[h].at[s - 1, p, t],
            send_sem=send_sem.at[h, s - 1, t, p], recv_sem=recv_sem.at[h, s - 1, t, p],
            device_id={"dev": partner(k)}, device_id_type=MESH)

    def send_sum(h, c):
        part = (pl.ds(c * IC, IC), pl.ds(base[h], size[h]))
        return pltpu.make_async_remote_copy(
            src_ref=v_rel.at[part], dst_ref=v_in.at[part],
            send_sem=vsend_sem.at[h, c], recv_sem=vrecv_sem.at[h, c],
            device_id={"dev": partner(second[h])}, device_id_type=MESH)

    def make_kron():
        spread = (iota((o * TILE, o), 0) // TILE == iota((o * TILE, o), 1)).astype(BF16)
        cor = jnp.dot(spread, cot[...], preferred_element_type=F32).astype(BF16)
        for h in range(2):
            def left(p0, np_):
                wide = 4 * np_ * TILE
                col = iota((n, wide), 1) // TILE
                slot = col // np_
                k = slot // 2 * first[h] + slot % 2
                dev = ((me // 4 + k // 4) % 2) * 4 + ((me // 2 + k // 2) % 2) * 2 + (me + k) % 2
                sel = (iota((n, wide), 0) == dev * rows_p + col % np_ + p0).astype(BF16)
                m = jnp.dot(cor, sel, preferred_element_type=F32)
                keep = iota((o * TILE, wide), 0) % TILE == iota((o * TILE, wide), 1) % TILE
                return jnp.where(keep, m, 0.0).astype(BF16)

            def full(g, _):
                kron[h, g] = left(g * PG, PG)
                return 0

            lax.fori_loop(0, rows_p // PG, full, 0)
            kron_last[h] = left(rows_p // PG * PG, rows_p % PG)

    def group(g, p0, np_):
        for h in range(2):
            def arrived(x, _):
                for s in range(1, 4):
                    for t in (1, 0):
                        send(h, s, t, p0 + x).wait_recv()
                return 0

            lax.fori_loop(0, np_, arrived, 0)

            def rhs(t, r0):
                tiles = [g_scr[pl.ds(p0, np_), partner(t * second[h]), pl.ds(base[h] + r0, TILE), :]]
                tiles += [recv[h][s, pl.ds(p0, np_), t, pl.ds(r0, TILE), :] for s in range(3)]
                return jnp.concatenate(tiles, 0).reshape(4 * np_ * TILE, LANES)

            def tile(r0, skip):
                left = kron[h, g] if np_ == PG else kron_last[h]
                out = jnp.dot(left, jnp.concatenate([rhs(0, r0), rhs(1, r0)], 1), preferred_element_type=F32)
                out = out.reshape(o, TILE, 2 * LANES)[:, skip:]
                at = pl.ds(base[h] + r0 + skip, TILE - skip)
                v_own[:, at, :] += out[:, :, :LANES]
                v_rel[:, at, :] += out[:, :, LANES:]

            def step(i, _):
                tile(pl.multiple_of(i * TILE, TILE), 0)
                return 0

            lax.fori_loop(0, size[h] // TILE, step, 0)
            if size[h] % TILE:
                tile(size[h] - TILE, TILE - size[h] % TILE)

    def row(p, _):
        rows_c = n // CHUNKS * o

        def second_step(c):
            h_scr[c * rows_c:(c + 1) * rows_c, :] = jnp.dot(t_scr[c % 2], cvp[...], preferred_element_type=F32)

        for c in range(CHUNKS):
            mine = range(c * nqb // CHUNKS, (c + 1) * nqb // CHUNKS)
            for x in mine:
                fetch(p, x).wait()
            pairs = len(mine) * QB // 2

            def first_step(i, _):
                q = c * pairs + i
                blk, r = q // (QB // 2), q % (QB // 2) * 2
                t = [jnp.dot(cot[...], abuf[blk, r + h], preferred_element_type=F32) for h in range(2)]
                at = pl.multiple_of(i * 2 * o, 2 * o)
                t_scr[c % 2, pl.ds(at, 2 * o), :] = jnp.concatenate(t, 0).astype(BF16)
                return 0

            lax.fori_loop(0, pairs, first_step, 0, unroll=True)
            if c:
                second_step(c - 1)
            for x in mine:
                fetch((p + 1) % rows_p, x).start()
        second_step(CHUNKS - 1)
        for j in range(0, o, 2):
            h = jnp.concatenate([h_scr[pl.ds(j + x, n, stride=o), :] for x in range(2)], 1).astype(BF16)
            g = jnp.dot(cvt[...], h, preferred_element_type=F32).astype(BF16)
            for x in range(2):
                d, r = divmod(j + x, od)
                g_scr[p, d, r * v:(r + 1) * v, :] = g[:, x * LANES:(x + 1) * LANES]
        for t in (1, 0):
            for s in (2, 3, 1):
                for h in range(2):
                    send(h, s, t, p).start()

        @pl.when(p == 0)
        def _():
            make_kron()
            v_own[...] = jnp.zeros_like(v_own)
            v_rel[...] = jnp.zeros_like(v_rel)

        @pl.when((p % PG == PG - 1) & (p > PG))
        def _():
            group(p // PG - 1, (p // PG - 1) * PG, PG)
        return 0

    lax.fori_loop(0, rows_p, row, 0)
    groups = rows_p // PG
    group(groups - 1, (groups - 1) * PG, PG)
    group(groups, groups * PG, rows_p % PG)
    def start_sum(c, _):
        for h in range(2):
            send_sum(h, c).start()
        return 0

    lax.fori_loop(0, o // IC, start_sum, 0)

    v_in[:, pts:, :] = jnp.zeros_like(v_in[:, pts:, :])
    evb = jnp.broadcast_to(evrow[...], (LANES, LANES))
    evsum = (evb + evb.T)[:v]

    def energies(c, _):
        for h in range(2):
            send_sum(h, c).wait_recv()

        def one(x, _):
            i = c * IC + x
            for j in range(od):
                at = pl.ds(j * v, LANES)
                x = v_own[i, at, :] + v_in[i, at, :]
                xt = x.T[:v]
                x = x[:v]
                e = x * (2.0 * x - xt) / (eo_ref[me * od + j] + eo_ref[i] - evsum)
                es[j, i] = jnp.sum(e.reshape(v // 8, 8, LANES), 0)
            return 0

        lax.fori_loop(0, IC, one, 0)
        return 0

    lax.fori_loop(0, o // IC, energies, 0)
    for j in range(od):
        e_ref[:, j:j + 1] = jnp.sum(jnp.sum(es[j], 1), 1, keepdims=True)

    for x in range(nqb):
        fetch(0, x).wait()

    def drain(p, _):
        for h in range(2):
            for s in range(1, 4):
                for t in range(2):
                    send(h, s, t, p).wait_send()
        return 0

    lax.fori_loop(0, rows_p, drain, 0)
    for c in range(o // IC):
        for h in range(2):
            send_sum(h, c).wait_send()


def solution(mesh):
    ndev = mesh.shape["dev"]

    def per_device(a_ints, c_occ, c_vir, eps_occ, eps_vir):
        rows_p, n = a_ints.shape[:2]
        o, v = c_occ.shape[1], c_vir.shape[1]
        od = o // ndev
        pts = od * v
        vm = pl.BlockSpec(memory_space=pltpu.VMEM)
        return pl.pallas_call(
            functools.partial(kernel, ndev),
            out_shape=jax.ShapeDtypeStruct((o, od), F32),
            in_specs=[pl.BlockSpec(memory_space=pl.ANY), vm, vm, pl.BlockSpec(memory_space=pltpu.SMEM), vm],
            out_specs=vm,
            scratch_shapes=[
                pltpu.VMEM((n // QB, QB, n, n), BF16),
                pltpu.VMEM((2, n // CHUNKS * o, n), BF16),
                pltpu.VMEM((n * o, LANES), F32),
                pltpu.VMEM((rows_p, ndev, pts, LANES), BF16),
                pltpu.VMEM((3, rows_p, 2, CUT, LANES), BF16),
                pltpu.VMEM((3, rows_p, 2, pts - CUT, LANES), BF16),
                pltpu.VMEM((o, pts + 8, LANES), F32),
                pltpu.VMEM((o, pts, LANES), F32),
                pltpu.VMEM((o, pts + 8, LANES), F32),
                pltpu.VMEM((2, 4, o * TILE, 16 * TILE), BF16),
                pltpu.VMEM((2, o * TILE, 8 * TILE), BF16),
                pltpu.VMEM((o, n), BF16),
                pltpu.VMEM((v, n), BF16),
                pltpu.VMEM((n, LANES), BF16),
                pltpu.VMEM((1, LANES), F32),
                pltpu.VMEM((od, o, 8, LANES), F32),
                pltpu.SemaphoreType.DMA((n // QB,)),
                pltpu.SemaphoreType.DMA((2, 3, 2, rows_p)),
                pltpu.SemaphoreType.DMA((2, 3, 2, rows_p)),
                pltpu.SemaphoreType.DMA((2, o // IC)),
                pltpu.SemaphoreType.DMA((2, o // IC)),
            ],
            compiler_params=pltpu.CompilerParams(
                collective_id=0, has_side_effects=True, vmem_limit_bytes=62 * 2**20),
        )(a_ints, c_occ, c_vir, eps_occ, eps_vir.reshape(1, v))

    return jax.shard_map(
        per_device,
        mesh=mesh,
        in_specs=(P(("frag", "dev")), P("frag"), P("frag"), P("frag"), P("frag")),
        out_specs=P("frag", "dev"),
        check_vma=False,
    )
```

```python
import functools

import jax
import jax.numpy as jnp
from jax import lax
from jax.experimental import pallas as pl
from jax.experimental.pallas import tpu as pltpu
from jax.sharding import PartitionSpec as P

MESH = pl.DeviceIdType.MESH
F32, BF16 = jnp.float32, jnp.bfloat16
NT = (((1,), (1,)), ((), ()))
LANES = 128
TILE = 16
QB = 16
CHUNKS = 3
IC = 4
CUT = 176
PG = 4
DEFER = 15


def iota(shape, dim):
    return lax.broadcasted_iota(jnp.int32, shape, dim)


def eye(n):
    return (iota((n, n), 0) == iota((n, n), 1)).astype(BF16)


def kernel(ndev, a_ref, co_ref, cv_ref, eo_ref, ev_ref, e_ref,
           abuf, t_scr, h_scr, g_scr, recv_a, recv_b, v_sum, v_in, kron, kron_last, cot, cvt, cvp, evrow, es,
           a_sem, send_sem, recv_sem, vsend_sem, vrecv_sem):
    rows_p, n = a_ref.shape[0], a_ref.shape[1]
    o, v = co_ref.shape[1], cv_ref.shape[1]
    od = o // ndev
    pts = od * v
    nqb = n // QB
    me = lax.axis_index("dev")
    recv = (recv_a, recv_b)
    cut = recv_a.shape[3]
    base = (0, cut)
    size = (cut, pts - cut)
    first = (2, 4)
    second = (4, 2)

    def partner(k):
        parts = [((me // s) % 2 + (k // s) % 2) % 2 * s for s in (4, 2, 1)]
        return parts[0] + parts[1] + parts[2]

    def slots(h):
        return (0, 1, first[h], first[h] + 1)

    def fetch(p, x):
        return pltpu.make_async_copy(a_ref.at[p, pl.ds(x * QB, QB)], abuf.at[x], a_sem.at[x])

    for x in range(nqb):
        fetch(0, x).start()

    barrier = pltpu.get_barrier_semaphore()
    for k in range(1, 6):
        pl.semaphore_signal(barrier, inc=1, device_id={"dev": partner(k)}, device_id_type=MESH)

    cot[...] = lax.dot_general(eye(o), co_ref[...], NT, preferred_element_type=F32).astype(BF16)
    cvt[...] = lax.dot_general(eye(v), cv_ref[...], NT, preferred_element_type=F32).astype(BF16)
    cvp[...] = jnp.zeros_like(cvp)
    cvp[:, :v] = cv_ref[...]
    evrow[...] = jnp.ones_like(evrow)
    evrow[:, :v] = ev_ref[...]

    pl.semaphore_wait(barrier, 5)

    def send(h, s, t, p):
        k = slots(h)[s]
        return pltpu.make_async_remote_copy(
            src_ref=g_scr.at[p, partner(k ^ (t * second[h])), pl.ds(base[h], size[h])],
            dst_ref=recv[h].at[s - 1, p, t],
            send_sem=send_sem.at[h, s - 1, t, p], recv_sem=recv_sem.at[h, s - 1, t, p],
            device_id={"dev": partner(k)}, device_id_type=MESH)

    def send_sum(h, c):
        part = (pl.ds(c * IC, IC), pl.ds(base[h], size[h]))
        return pltpu.make_async_remote_copy(
            src_ref=v_sum.at[(1,) + part], dst_ref=v_in.at[part],
            send_sem=vsend_sem.at[h, c], recv_sem=vrecv_sem.at[h, c],
            device_id={"dev": partner(second[h])}, device_id_type=MESH)

    def make_kron():
        spread = (iota((o * TILE, o), 0) // TILE == iota((o * TILE, o), 1)).astype(BF16)
        cor = jnp.dot(spread, cot[...], preferred_element_type=F32).astype(BF16)
        for h in range(2):
            def left(p0, np_):
                wide = 4 * np_ * TILE
                col = iota((n, wide), 1) // TILE
                slot = col // np_
                k = slot // 2 * first[h] + slot % 2
                dev = ((me // 4 + k // 4) % 2) * 4 + ((me // 2 + k // 2) % 2) * 2 + (me + k) % 2
                sel = (iota((n, wide), 0) == dev * rows_p + col % np_ + p0).astype(BF16)
                m = jnp.dot(cor, sel, preferred_element_type=F32)
                keep = iota((o * TILE, wide), 0) % TILE == iota((o * TILE, wide), 1) % TILE
                return jnp.where(keep, m, 0.0).astype(BF16)

            def full(g, _):
                kron[h, g] = left(g * PG, PG)
                return 0

            lax.fori_loop(0, rows_p // PG, full, 0)
            kron_last[h] = left(rows_p // PG * PG, rows_p % PG)

    def group(t, g, p0, np_):
        for h in range(2):
            def arrived(x, _):
                for s in range(1, 4):
                    send(h, s, t, p0 + x).wait_recv()
                return 0

            lax.fori_loop(0, np_, arrived, 0)

            def rhs(r0):
                tiles = [g_scr[pl.ds(p0, np_), partner(t * second[h]), pl.ds(base[h] + r0, TILE), :]]
                tiles += [recv[h][s, pl.ds(p0, np_), t, pl.ds(r0, TILE), :] for s in range(3)]
                return jnp.concatenate(tiles, 0).reshape(4 * np_ * TILE, LANES)

            def tiles(*where):
                left = kron[h, g] if np_ == PG else kron_last[h]
                right = [rhs(r0) for r0, _ in where]
                out = jnp.dot(left, jnp.concatenate(right, 1), preferred_element_type=F32)
                out = out.reshape(o, TILE, len(where) * LANES)
                for x, (r0, skip) in enumerate(where):
                    at = pl.ds(base[h] + r0 + skip, TILE - skip)
                    v_sum[t, :, at, :] += out[:, skip:, x * LANES:(x + 1) * LANES]

            def step(i, _):
                r0 = pl.multiple_of(i * 2 * TILE, 2 * TILE)
                tiles((r0, 0), (r0 + TILE, 0))
                return 0

            pairs = size[h] // (2 * TILE)
            lax.fori_loop(0, pairs, step, 0, unroll=True)
            rest = [(r0, 0) for r0 in range(pairs * 2 * TILE, size[h] - TILE + 1, TILE)]
            if size[h] % TILE:
                rest.append((size[h] - TILE, TILE - size[h] % TILE))
            if rest:
                tiles(*rest)

    def late(p, _):
        for s in (2, 3, 1):
            for h in range(2):
                send(h, s, 0, p).start()
        return 0

    def row(p, _):
        rows_c = n // CHUNKS * o

        def second_step(c):
            h_scr[c * rows_c:(c + 1) * rows_c, :] = jnp.dot(t_scr[c % 2], cvp[...], preferred_element_type=F32)

        for c in range(CHUNKS):
            mine = range(c * nqb // CHUNKS, (c + 1) * nqb // CHUNKS)
            for x in mine:
                fetch(p, x).wait()
            pairs = len(mine) * QB // 2

            def first_step(i, _):
                q = c * pairs + i
                blk, r = q // (QB // 2), q % (QB // 2) * 2
                t = [jnp.dot(cot[...], abuf[blk, r + h], preferred_element_type=F32) for h in range(2)]
                at = pl.multiple_of(i * 2 * o, 2 * o)
                t_scr[c % 2, pl.ds(at, 2 * o), :] = jnp.concatenate(t, 0).astype(BF16)
                return 0

            lax.fori_loop(0, pairs, first_step, 0, unroll=True)
            if c:
                second_step(c - 1)
            for x in mine:
                fetch((p + 1) % rows_p, x).start()
        second_step(CHUNKS - 1)
        for j in range(0, o, 2):
            h = jnp.concatenate([h_scr[pl.ds(j + x, n, stride=o), :] for x in range(2)], 1).astype(BF16)
            g = jnp.dot(cvt[...], h, preferred_element_type=F32).astype(BF16)
            for x in range(2):
                d, r = divmod(j + x, od)
                g_scr[p, d, r * v:(r + 1) * v, :] = g[:, x * LANES:(x + 1) * LANES]
        for s in (2, 3, 1):
            for h in range(2):
                send(h, s, 1, p).start()

        @pl.when(p < DEFER)
        def _():
            late(p, 0)

        @pl.when(p == 0)
        def _():
            make_kron()
            v_sum[...] = jnp.zeros_like(v_sum)

        @pl.when((p % PG == PG - 1) & (p > PG))
        def _():
            g = p // PG - 1

            def target(t, _):
                group(t, g, g * PG, PG)
                return 0

            lax.fori_loop(0, 2, target, 0)
        return 0

    lax.fori_loop(0, rows_p, row, 0)
    lax.fori_loop(DEFER, rows_p, late, 0)
    groups = rows_p // PG

    def finish(u, _):
        group(1 - u, groups - 1, (groups - 1) * PG, PG)
        group(1 - u, groups, groups * PG, rows_p % PG)

        @pl.when(u == 0)
        def _():
            def start_sum(c, _):
                for h in range(2):
                    send_sum(h, c).start()
                return 0

            lax.fori_loop(0, o // IC, start_sum, 0)
        return 0

    lax.fori_loop(0, 2, finish, 0)

    v_in[:, pts:, :] = jnp.zeros_like(v_in[:, pts:, :])
    evb = jnp.broadcast_to(evrow[...], (LANES, LANES))
    evsum = (evb + evb.T)[:v]

    def energies(c, _):
        for h in range(2):
            send_sum(h, c).wait_recv()

        def one(x, _):
            i = c * IC + x
            for j in range(od):
                at = pl.ds(j * v, LANES)
                x = v_sum[0, i, at, :] + v_in[i, at, :]
                xt = x.T[:v]
                x = x[:v]
                e = x * (2.0 * x - xt) / (eo_ref[me * od + j] + eo_ref[i] - evsum)
                es[j, i] = jnp.sum(e.reshape(v // 8, 8, LANES), 0)
            return 0

        lax.fori_loop(0, IC, one, 0)
        return 0

    lax.fori_loop(0, o // IC, energies, 0)
    for j in range(od):
        e_ref[:, j:j + 1] = jnp.sum(jnp.sum(es[j], 1), 1, keepdims=True)

    for x in range(nqb):
        fetch(0, x).wait()

    def drain(p, _):
        for h in range(2):
            for s in range(1, 4):
                for t in range(2):
                    send(h, s, t, p).wait_send()
        return 0

    lax.fori_loop(0, rows_p, drain, 0)
    for c in range(o // IC):
        for h in range(2):
            send_sum(h, c).wait_send()


def solution(mesh):
    ndev = mesh.shape["dev"]

    def per_device(a_ints, c_occ, c_vir, eps_occ, eps_vir):
        rows_p, n = a_ints.shape[:2]
        o, v = c_occ.shape[1], c_vir.shape[1]
        od = o // ndev
        pts = od * v
        vm = pl.BlockSpec(memory_space=pltpu.VMEM)
        return pl.pallas_call(
            functools.partial(kernel, ndev),
            out_shape=jax.ShapeDtypeStruct((o, od), F32),
            in_specs=[pl.BlockSpec(memory_space=pl.ANY), vm, vm, pl.BlockSpec(memory_space=pltpu.SMEM), vm],
            out_specs=vm,
            scratch_shapes=[
                pltpu.VMEM((n // QB, QB, n, n), BF16),
                pltpu.VMEM((2, n // CHUNKS * o, n), BF16),
                pltpu.VMEM((n * o, LANES), F32),
                pltpu.VMEM((rows_p, ndev, pts, LANES), BF16),
                pltpu.VMEM((3, rows_p, 2, CUT, LANES), BF16),
                pltpu.VMEM((3, rows_p, 2, pts - CUT, LANES), BF16),
                pltpu.VMEM((2, o, pts + 8, LANES), F32),
                pltpu.VMEM((o, pts + 8, LANES), F32),
                pltpu.VMEM((2, 4, o * TILE, 16 * TILE), BF16),
                pltpu.VMEM((2, o * TILE, 8 * TILE), BF16),
                pltpu.VMEM((o, n), BF16),
                pltpu.VMEM((v, n), BF16),
                pltpu.VMEM((n, LANES), BF16),
                pltpu.VMEM((1, LANES), F32),
                pltpu.VMEM((od, o, 8, LANES), F32),
                pltpu.SemaphoreType.DMA((n // QB,)),
                pltpu.SemaphoreType.DMA((2, 3, 2, rows_p)),
                pltpu.SemaphoreType.DMA((2, 3, 2, rows_p)),
                pltpu.SemaphoreType.DMA((2, o // IC)),
                pltpu.SemaphoreType.DMA((2, o // IC)),
            ],
            compiler_params=pltpu.CompilerParams(
                collective_id=0, has_side_effects=True, vmem_limit_bytes=62 * 2**20),
        )(a_ints, c_occ, c_vir, eps_occ, eps_vir.reshape(1, v))

    return jax.shard_map(
        per_device,
        mesh=mesh,
        in_specs=(P(("frag", "dev")), P("frag"), P("frag"), P("frag"), P("frag")),
        out_specs=P("frag", "dev"),
        check_vma=False,
    )
```

```python
import functools

import jax
import jax.numpy as jnp
from jax import lax
from jax.experimental import pallas as pl
from jax.experimental.pallas import tpu as pltpu
from jax.sharding import PartitionSpec as P

MESH = pl.DeviceIdType.MESH
F32, BF16 = jnp.float32, jnp.bfloat16
NT = (((1,), (1,)), ((), ()))
LANES = 128
TILE = 16
QB = 16
CHUNKS = 3
IC = 4
CUT = 176
PG = 4
DEFER = 16


def iota(shape, dim):
    return lax.broadcasted_iota(jnp.int32, shape, dim)


def eye(n):
    return (iota((n, n), 0) == iota((n, n), 1)).astype(BF16)


def kernel(ndev, a_ref, cot, cv_ref, eo_ref, ev_ref, e_ref,
           abuf, t_scr, h_scr, g_scr, recv_a, recv_b, v_sum, v_in, kron, kron_last, cvt, cvp, evrow, es,
           a_sem, send_sem, recv_sem, vsend_sem, vrecv_sem):
    rows_p, n = a_ref.shape[0], a_ref.shape[1]
    o, v = cot.shape[0], cv_ref.shape[1]
    od = o // ndev
    pts = od * v - TILE
    nqb = n // QB
    me = lax.axis_index("dev")
    recv = (recv_a, recv_b)
    cut = recv_a.shape[3]
    base = (0, cut)
    size = (cut, pts - cut)
    first = (2, 4)
    second = (4, 2)

    def partner(k):
        parts = [((me // s) % 2 + (k // s) % 2) % 2 * s for s in (4, 2, 1)]
        return parts[0] + parts[1] + parts[2]

    def slots(h):
        return (0, 1, first[h], first[h] + 1)

    def fetch(p, x):
        return pltpu.make_async_copy(a_ref.at[p, pl.ds(x * QB, QB)], abuf.at[x], a_sem.at[x])

    for x in range(nqb):
        fetch(0, x).start()

    barrier = pltpu.get_barrier_semaphore()
    for k in range(1, 6):
        pl.semaphore_signal(barrier, inc=1, device_id={"dev": partner(k)}, device_id_type=MESH)

    cvt[...] = lax.dot_general(eye(v), cv_ref[...], NT, preferred_element_type=F32).astype(BF16)
    cvp[...] = jnp.zeros_like(cvp)
    cvp[:, :v] = cv_ref[...]
    evrow[...] = jnp.ones_like(evrow)
    evrow[:, :v] = ev_ref[...]

    def send(h, s, t, p):
        k = slots(h)[s]
        return pltpu.make_async_remote_copy(
            src_ref=g_scr.at[p, partner(k ^ (t * second[h])), pl.ds(base[h], size[h])],
            dst_ref=recv[h].at[s - 1, p, t],
            send_sem=send_sem.at[h, s - 1, t, p], recv_sem=recv_sem.at[h, s - 1, t, p],
            device_id={"dev": partner(k)}, device_id_type=MESH)

    def send_sum(h, c):
        part = (pl.ds(c * IC, IC), pl.ds(base[h], size[h]))
        return pltpu.make_async_remote_copy(
            src_ref=v_sum.at[(1,) + part], dst_ref=v_in.at[part],
            send_sem=vsend_sem.at[h, c], recv_sem=vrecv_sem.at[h, c],
            device_id={"dev": partner(second[h])}, device_id_type=MESH)

    spare = LANES - v
    lane = iota((TILE, LANES), 1)

    def pack(blocks):
        extra = blocks[-1][v - TILE:]
        rows = jnp.concatenate(blocks, 0)[:pts]
        moved = [jnp.where(lane < v, rows[m * TILE:(m + 1) * TILE], pltpu.roll(extra, v - m * spare, 1))
                 for m in range(v // spare)]
        return jnp.concatenate(moved + [rows[v // spare * TILE:]], 0)

    def unpack(rows):
        extra = jnp.zeros((TILE, LANES), F32)
        for m in range(v // spare):
            x = pltpu.roll(rows[m * TILE:(m + 1) * TILE], LANES - v + m * spare, 1)
            extra = jnp.where((lane >= m * spare) & (lane < (m + 1) * spare), x, extra)
        rows = jnp.where(iota(rows.shape, 1) < v, rows, 0.0)
        return jnp.concatenate([rows, extra], 0)

    def make_kron():
        spread = (iota((o * TILE, o), 0) // TILE == iota((o * TILE, o), 1)).astype(BF16)
        cor = jnp.dot(spread, cot[...], preferred_element_type=F32).astype(BF16)
        for h in range(2):
            def left(p0, np_):
                wide = 4 * np_ * TILE
                col = iota((n, wide), 1) // TILE
                slot = col // np_
                k = slot // 2 * first[h] + slot % 2
                dev = ((me // 4 + k // 4) % 2) * 4 + ((me // 2 + k // 2) % 2) * 2 + (me + k) % 2
                sel = (iota((n, wide), 0) == dev * rows_p + col % np_ + p0).astype(BF16)
                m = jnp.dot(cor, sel, preferred_element_type=F32)
                keep = iota((o * TILE, wide), 0) % TILE == iota((o * TILE, wide), 1) % TILE
                return jnp.where(keep, m, 0.0).astype(BF16)

            def full(g, _):
                kron[h, g] = left(g * PG, PG)
                return 0

            lax.fori_loop(0, rows_p // PG, full, 0)
            kron_last[h] = left(rows_p // PG * PG, rows_p % PG)

    def group(t, g, p0, np_):
        for h in range(2):
            def arrived(x, _):
                for s in range(1, 4):
                    send(h, s, t, p0 + x).wait_recv()
                return 0

            lax.fori_loop(0, np_, arrived, 0)

            def rhs(r0):
                tiles = [g_scr[pl.ds(p0, np_), partner(t * second[h]), pl.ds(base[h] + r0, TILE), :]]
                tiles += [recv[h][s, pl.ds(p0, np_), t, pl.ds(r0, TILE), :] for s in range(3)]
                return jnp.concatenate(tiles, 0).reshape(4 * np_ * TILE, LANES)

            def tiles(*where):
                left = kron[h, g] if np_ == PG else kron_last[h]
                right = [rhs(r0) for r0, _ in where]
                out = jnp.dot(left, jnp.concatenate(right, 1), preferred_element_type=F32)
                out = out.reshape(o, TILE, len(where) * LANES)
                for x, (r0, skip) in enumerate(where):
                    at = pl.ds(base[h] + r0 + skip, TILE - skip)
                    v_sum[t, :, at, :] += out[:, skip:, x * LANES:(x + 1) * LANES]

            def step(i, _):
                r0 = pl.multiple_of(i * 2 * TILE, 2 * TILE)
                tiles((r0, 0), (r0 + TILE, 0))
                return 0

            pairs = size[h] // (2 * TILE)
            lax.fori_loop(0, pairs, step, 0, unroll=True)
            rest = [(r0, 0) for r0 in range(pairs * 2 * TILE, size[h] - TILE + 1, TILE)]
            if size[h] % TILE:
                rest.append((size[h] - TILE, TILE - size[h] % TILE))
            if rest:
                tiles(*rest)

    def late(p, _):
        for s in (2, 3, 1):
            for h in range(2):
                send(h, s, 0, p).start()
        return 0

    def row(p, _):
        rows_c = n // CHUNKS * o

        def second_step(c):
            h_scr[c * rows_c:(c + 1) * rows_c, :] = jnp.dot(t_scr[c % 2], cvp[...], preferred_element_type=F32)

        for c in range(CHUNKS):
            mine = range(c * nqb // CHUNKS, (c + 1) * nqb // CHUNKS)
            for x in mine:
                fetch(p, x).wait()
            pairs = len(mine) * QB // 2

            def first_step(i, _):
                q = c * pairs + i
                blk, r = q // (QB // 2), q % (QB // 2) * 2
                t = [jnp.dot(cot[...], abuf[blk, r + h], preferred_element_type=F32) for h in range(2)]
                at = pl.multiple_of(i * 2 * o, 2 * o)
                t_scr[c % 2, pl.ds(at, 2 * o), :] = jnp.concatenate(t, 0).astype(BF16)
                return 0

            lax.fori_loop(0, pairs, first_step, 0, unroll=True)
            if c:
                second_step(c - 1)
            for x in mine:
                fetch((p + 1) % rows_p, x).start()
        second_step(CHUNKS - 1)
        for d in range(0, ndev, 2):
            h = jnp.concatenate([h_scr[pl.ds(d * od + x, n, stride=o), :] for x in range(2 * od)], 1).astype(BF16)
            g = jnp.dot(cvt[...], h, preferred_element_type=F32)
            g = [g[:, x * LANES:(x + 1) * LANES] for x in range(2 * od)]
            for x in range(2):
                g_scr[p, d + x] = pack(g[x * od:(x + 1) * od]).astype(BF16)
        for s in (2, 3, 1):
            for h in range(2):
                send(h, s, 1, p).start()

        @pl.when(p < DEFER)
        def _():
            late(p, 0)

        @pl.when((p % PG == 1) & (p > PG))
        def _():
            g = p // PG - 1
            group(1, g, g * PG, PG)
        return 0

    make_kron()
    v_sum[...] = jnp.zeros_like(v_sum)
    pl.semaphore_wait(barrier, 5)
    lax.fori_loop(0, rows_p, row, 0)
    lax.fori_loop(DEFER, rows_p, late, 0)
    groups = rows_p // PG
    group(1, groups, groups * PG, rows_p % PG)

    def start_sum(c, _):
        for h in range(2):
            send_sum(h, c).start()
        return 0

    lax.fori_loop(0, o // IC, start_sum, 0)

    def own(g, _):
        group(0, g, g * PG, PG)
        return 0

    lax.fori_loop(0, groups, own, 0)
    group(0, groups, groups * PG, rows_p % PG)

    evb = jnp.broadcast_to(evrow[...], (LANES, LANES))
    evsum = (evb + evb.T)[:v]

    def energies(c, _):
        for h in range(2):
            send_sum(h, c).wait_recv()

        def one(x, _):
            i = c * IC + x
            full = unpack(v_sum[0, i] + v_in[i])
            for j in range(od):
                x = full[j * v:(j + 1) * v]
                xt = jnp.concatenate([x, jnp.zeros((spare, LANES), F32)], 0).T[:v]
                e = x * (2.0 * x - xt) / (eo_ref[me * od + j] + eo_ref[i] - evsum)
                es[j, i] = jnp.sum(e.reshape(v // 8, 8, LANES), 0)
            return 0

        lax.fori_loop(0, IC, one, 0)
        return 0

    lax.fori_loop(0, o // IC, energies, 0)
    for j in range(od):
        e_ref[:, j:j + 1] = jnp.sum(jnp.sum(es[j], 1), 1, keepdims=True)

    for x in range(nqb):
        fetch(0, x).wait()

    def drain(p, _):
        for h in range(2):
            for s in range(1, 4):
                for t in range(2):
                    send(h, s, t, p).wait_send()
        return 0

    lax.fori_loop(0, rows_p, drain, 0)
    for c in range(o // IC):
        for h in range(2):
            send_sum(h, c).wait_send()


def solution(mesh):
    ndev = mesh.shape["dev"]

    def per_device(a_ints, c_occ, c_vir, eps_occ, eps_vir):
        rows_p, n = a_ints.shape[:2]
        o, v = c_occ.shape[1], c_vir.shape[1]
        od = o // ndev
        pts = od * v - TILE
        vm = pl.BlockSpec(memory_space=pltpu.VMEM)
        return pl.pallas_call(
            functools.partial(kernel, ndev),
            out_shape=jax.ShapeDtypeStruct((o, od), F32),
            in_specs=[pl.BlockSpec(memory_space=pl.ANY), vm, vm, pl.BlockSpec(memory_space=pltpu.SMEM), vm],
            out_specs=vm,
            scratch_shapes=[
                pltpu.VMEM((n // QB, QB, n, n), BF16),
                pltpu.VMEM((2, n // CHUNKS * o, n), BF16),
                pltpu.VMEM((n * o, LANES), F32),
                pltpu.VMEM((rows_p, ndev, pts, LANES), BF16),
                pltpu.VMEM((3, rows_p, 2, CUT, LANES), BF16),
                pltpu.VMEM((3, rows_p, 2, pts - CUT, LANES), BF16),
                pltpu.VMEM((2, o, pts, LANES), F32),
                pltpu.VMEM((o, pts, LANES), F32),
                pltpu.VMEM((2, 4, o * TILE, 16 * TILE), BF16),
                pltpu.VMEM((2, o * TILE, 8 * TILE), BF16),
                pltpu.VMEM((v, n), BF16),
                pltpu.VMEM((n, LANES), BF16),
                pltpu.VMEM((1, LANES), F32),
                pltpu.VMEM((od, o, 8, LANES), F32),
                pltpu.SemaphoreType.DMA((n // QB,)),
                pltpu.SemaphoreType.DMA((2, 3, 2, rows_p)),
                pltpu.SemaphoreType.DMA((2, 3, 2, rows_p)),
                pltpu.SemaphoreType.DMA((2, o // IC)),
                pltpu.SemaphoreType.DMA((2, o // IC)),
            ],
            compiler_params=pltpu.CompilerParams(
                collective_id=0, has_side_effects=True, vmem_limit_bytes=62 * 2**20),
        )(a_ints, c_occ.T, c_vir, eps_occ, eps_vir.reshape(1, v))

    return jax.shard_map(
        per_device,
        mesh=mesh,
        in_specs=(P(("frag", "dev")), P("frag"), P("frag"), P("frag"), P("frag")),
        out_specs=P("frag", "dev"),
        check_vma=False,
    )
```

```python
import functools

import jax
import jax.numpy as jnp
from jax import lax
from jax.experimental import pallas as pl
from jax.experimental.pallas import tpu as pltpu
from jax.sharding import PartitionSpec as P

MESH = pl.DeviceIdType.MESH
F32, BF16 = jnp.float32, jnp.bfloat16
NT = (((1,), (1,)), ((), ()))
LANES = 128
TILE = 16
QB = 16
CHUNKS = 3
IC = 4
CUT = 176
PG = 4
DEFER = 16


def iota(shape, dim):
    return lax.broadcasted_iota(jnp.int32, shape, dim)


def eye(n):
    return (iota((n, n), 0) == iota((n, n), 1)).astype(BF16)


def kernel(ndev, a_ref, cot, cv_ref, eo_ref, ev_ref, e_ref,
           abuf, t_scr, h_scr, g_scr, recv_a, recv_b, v_sum, v_in, kron, kron_last, cvt, cvp, evrow, es,
           a_sem, send_sem, recv_sem, vsend_sem, vrecv_sem):
    rows_p, n = a_ref.shape[0], a_ref.shape[1]
    o, v = cot.shape[0], cv_ref.shape[1]
    od = o // ndev
    pts = od * v - TILE
    nqb = n // QB
    me = lax.axis_index("dev")
    recv = (recv_a, recv_b)
    cut = recv_a.shape[3]
    base = (0, cut)
    size = (cut, pts - cut)
    first = (2, 4)
    second = (4, 2)

    def partner(k):
        parts = [((me // s) % 2 + (k // s) % 2) % 2 * s for s in (4, 2, 1)]
        return parts[0] + parts[1] + parts[2]

    def slots(h):
        return (0, 1, first[h], first[h] + 1)

    def fetch(p, x):
        return pltpu.make_async_copy(a_ref.at[p, pl.ds(x * QB, QB)], abuf.at[x], a_sem.at[x])

    for x in range(nqb):
        fetch(0, x).start()

    barrier = pltpu.get_barrier_semaphore()
    for k in range(1, 6):
        pl.semaphore_signal(barrier, inc=1, device_id={"dev": partner(k)}, device_id_type=MESH)

    cvt[...] = lax.dot_general(eye(v), cv_ref[...], NT, preferred_element_type=F32).astype(BF16)
    cvp[...] = jnp.zeros_like(cvp)
    cvp[:, :v] = cv_ref[...]
    evrow[...] = jnp.ones_like(evrow)
    evrow[:, :v] = ev_ref[...]

    def send(h, s, t, p):
        k = slots(h)[s]
        return pltpu.make_async_remote_copy(
            src_ref=g_scr.at[p, partner(k ^ (t * second[h])), pl.ds(base[h], size[h])],
            dst_ref=recv[h].at[s - 1, p, t],
            send_sem=send_sem.at[h, s - 1, t, p], recv_sem=recv_sem.at[h, s - 1, t, p],
            device_id={"dev": partner(k)}, device_id_type=MESH)

    def send_sum(h, c):
        part = (pl.ds(c * IC, IC), pl.ds(base[h], size[h]))
        return pltpu.make_async_remote_copy(
            src_ref=v_sum.at[(1,) + part], dst_ref=v_in.at[part],
            send_sem=vsend_sem.at[h, c], recv_sem=vrecv_sem.at[h, c],
            device_id={"dev": partner(second[h])}, device_id_type=MESH)

    spare = LANES - v
    lane = iota((TILE, LANES), 1)

    def pack(blocks):
        extra = blocks[-1][v - TILE:]
        rows = jnp.concatenate(blocks, 0)[:pts]
        moved = [jnp.where(lane < v, rows[m * TILE:(m + 1) * TILE], pltpu.roll(extra, v - m * spare, 1))
                 for m in range(v // spare)]
        return jnp.concatenate(moved + [rows[v // spare * TILE:]], 0)

    def unpack(rows):
        extra = jnp.zeros((TILE, LANES), F32)
        for m in range(v // spare):
            x = pltpu.roll(rows[m * TILE:(m + 1) * TILE], LANES - v + m * spare, 1)
            extra = jnp.where((lane >= m * spare) & (lane < (m + 1) * spare), x, extra)
        rows = jnp.where(iota(rows.shape, 1) < v, rows, 0.0)
        return jnp.concatenate([rows, extra], 0)

    def make_kron():
        spread = (iota((o * TILE, o), 0) // TILE == iota((o * TILE, o), 1)).astype(BF16)
        cor = jnp.dot(spread, cot[...], preferred_element_type=F32).astype(BF16)
        for h in range(2):
            def left(p0, np_):
                wide = 4 * np_ * TILE
                col = iota((n, wide), 1) // TILE
                slot = col // np_
                k = slot // 2 * first[h] + slot % 2
                dev = ((me // 4 + k // 4) % 2) * 4 + ((me // 2 + k // 2) % 2) * 2 + (me + k) % 2
                sel = (iota((n, wide), 0) == dev * rows_p + col % np_ + p0).astype(BF16)
                m = jnp.dot(cor, sel, preferred_element_type=F32)
                keep = iota((o * TILE, wide), 0) % TILE == iota((o * TILE, wide), 1) % TILE
                return jnp.where(keep, m, 0.0).astype(BF16)

            def full(g, _):
                kron[h, g] = left(g * PG, PG)
                return 0

            lax.fori_loop(0, rows_p // PG, full, 0)
            kron_last[h] = left(rows_p // PG * PG, rows_p % PG)

    def group(t, g, p0, np_):
        for h in range(2):
            def arrived(x, _):
                for s in range(1, 4):
                    send(h, s, t, p0 + x).wait_recv()
                return 0

            lax.fori_loop(0, np_, arrived, 0)

            def rhs(r0):
                tiles = [g_scr[pl.ds(p0, np_), partner(t * second[h]), pl.ds(base[h] + r0, TILE), :]]
                tiles += [recv[h][s, pl.ds(p0, np_), t, pl.ds(r0, TILE), :] for s in range(3)]
                return jnp.concatenate(tiles, 0).reshape(4 * np_ * TILE, LANES)

            def tiles(*where):
                left = kron[h, g] if np_ == PG else kron_last[h]
                right = [rhs(r0) for r0, _ in where]
                out = jnp.dot(left, jnp.concatenate(right, 1), preferred_element_type=F32)
                out = out.reshape(o, TILE, len(where) * LANES)
                for x, (r0, skip) in enumerate(where):
                    at = pl.ds(base[h] + r0 + skip, TILE - skip)
                    v_sum[t, :, at, :] += out[:, skip:, x * LANES:(x + 1) * LANES]

            def step(i, _):
                r0 = pl.multiple_of(i * 2 * TILE, 2 * TILE)
                tiles((r0, 0), (r0 + TILE, 0))
                return 0

            pairs = size[h] // (2 * TILE)
            lax.fori_loop(0, pairs, step, 0, unroll=True)
            rest = [(r0, 0) for r0 in range(pairs * 2 * TILE, size[h] - TILE + 1, TILE)]
            if size[h] % TILE:
                rest.append((size[h] - TILE, TILE - size[h] % TILE))
            if rest:
                tiles(*rest)

    def late(p, _):
        for s in (2, 3, 1):
            for h in range(2):
                send(h, s, 0, p).start()
        return 0

    def row(p, _):
        rows_c = n // CHUNKS * o

        def second_step(c):
            h_scr[c * rows_c:(c + 1) * rows_c, :] = jnp.dot(t_scr[c % 2], cvp[...], preferred_element_type=F32)

        for c in range(CHUNKS):
            mine = range(c * nqb // CHUNKS, (c + 1) * nqb // CHUNKS)
            for x in mine:
                fetch(p, x).wait()
            pairs = len(mine) * QB // 2

            def first_step(i, _):
                q = c * pairs + i
                blk, r = q // (QB // 2), q % (QB // 2) * 2
                t = [jnp.dot(cot[...], abuf[blk, r + h], preferred_element_type=F32) for h in range(2)]
                at = pl.multiple_of(i * 2 * o, 2 * o)
                t_scr[c % 2, pl.ds(at, 2 * o), :] = jnp.concatenate(t, 0).astype(BF16)
                return 0

            lax.fori_loop(0, pairs, first_step, 0, unroll=True)
            if c:
                second_step(c - 1)
            for x in mine:
                fetch((p + 1) % rows_p, x).start()
        second_step(CHUNKS - 1)
        for d in range(0, ndev, 2):
            h = jnp.concatenate([h_scr[pl.ds(d * od + x, n, stride=o), :] for x in range(2 * od)], 1).astype(BF16)
            g = jnp.dot(cvt[...], h, preferred_element_type=F32)
            g = g.astype(BF16)
            g = [g[:, x * LANES:(x + 1) * LANES] for x in range(2 * od)]
            for x in range(2):
                g_scr[p, d + x] = pack(g[x * od:(x + 1) * od])
        for s in (2, 3, 1):
            for h in range(2):
                send(h, s, 1, p).start()

        @pl.when(p < DEFER)
        def _():
            late(p, 0)

        @pl.when((p % PG == 1) & (p > PG))
        def _():
            g = p // PG - 1
            group(1, g, g * PG, PG)
        return 0

    make_kron()
    v_sum[...] = jnp.zeros_like(v_sum)
    pl.semaphore_wait(barrier, 5)
    lax.fori_loop(0, rows_p, row, 0)
    lax.fori_loop(DEFER, rows_p, late, 0)
    groups = rows_p // PG
    group(1, groups, groups * PG, rows_p % PG)

    def start_sum(c, _):
        for h in range(2):
            send_sum(h, c).start()
        return 0

    lax.fori_loop(0, o // IC, start_sum, 0)

    def own(g, _):
        group(0, g, g * PG, PG)
        return 0

    lax.fori_loop(0, groups, own, 0)
    group(0, groups, groups * PG, rows_p % PG)

    evb = jnp.broadcast_to(evrow[...], (LANES, LANES))
    evsum = (evb + evb.T)[:v]

    def energies(c, _):
        for h in range(2):
            send_sum(h, c).wait_recv()

        def one(x, _):
            i = c * IC + x
            full = unpack(v_sum[0, i] + v_in[i])
            for j in range(od):
                x = full[j * v:(j + 1) * v]
                xt = jnp.concatenate([x, jnp.zeros((spare, LANES), F32)], 0).T[:v]
                e = x * (2.0 * x - xt) / (eo_ref[me * od + j] + eo_ref[i] - evsum)
                es[j, i] = jnp.sum(e.reshape(v // 8, 8, LANES), 0)
            return 0

        lax.fori_loop(0, IC, one, 0, unroll=True)
        return 0

    lax.fori_loop(0, o // IC, energies, 0)
    for j in range(od):
        e_ref[:, j:j + 1] = jnp.sum(jnp.sum(es[j], 1), 1, keepdims=True)

    for x in range(nqb):
        fetch(0, x).wait()

    def drain(p, _):
        for h in range(2):
            for s in range(1, 4):
                for t in range(2):
                    send(h, s, t, p).wait_send()
        return 0

    lax.fori_loop(0, rows_p, drain, 0)
    for c in range(o // IC):
        for h in range(2):
            send_sum(h, c).wait_send()


def solution(mesh):
    ndev = mesh.shape["dev"]

    def per_device(a_ints, c_occ, c_vir, eps_occ, eps_vir):
        rows_p, n = a_ints.shape[:2]
        o, v = c_occ.shape[1], c_vir.shape[1]
        od = o // ndev
        pts = od * v - TILE
        vm = pl.BlockSpec(memory_space=pltpu.VMEM)
        return pl.pallas_call(
            functools.partial(kernel, ndev),
            out_shape=jax.ShapeDtypeStruct((o, od), F32),
            in_specs=[pl.BlockSpec(memory_space=pl.ANY), vm, vm, pl.BlockSpec(memory_space=pltpu.SMEM), vm],
            out_specs=vm,
            scratch_shapes=[
                pltpu.VMEM((n // QB, QB, n, n), BF16),
                pltpu.VMEM((2, n // CHUNKS * o, n), BF16),
                pltpu.VMEM((n * o, LANES), F32),
                pltpu.VMEM((rows_p, ndev, pts, LANES), BF16),
                pltpu.VMEM((3, rows_p, 2, CUT, LANES), BF16),
                pltpu.VMEM((3, rows_p, 2, pts - CUT, LANES), BF16),
                pltpu.VMEM((2, o, pts, LANES), F32),
                pltpu.VMEM((o, pts, LANES), F32),
                pltpu.VMEM((2, 4, o * TILE, 16 * TILE), BF16),
                pltpu.VMEM((2, o * TILE, 8 * TILE), BF16),
                pltpu.VMEM((v, n), BF16),
                pltpu.VMEM((n, LANES), BF16),
                pltpu.VMEM((1, LANES), F32),
                pltpu.VMEM((od, o, 8, LANES), F32),
                pltpu.SemaphoreType.DMA((n // QB,)),
                pltpu.SemaphoreType.DMA((2, 3, 2, rows_p)),
                pltpu.SemaphoreType.DMA((2, 3, 2, rows_p)),
                pltpu.SemaphoreType.DMA((2, o // IC)),
                pltpu.SemaphoreType.DMA((2, o // IC)),
            ],
            compiler_params=pltpu.CompilerParams(
                collective_id=0, has_side_effects=True, vmem_limit_bytes=62 * 2**20),
        )(a_ints, c_occ.T, c_vir, eps_occ, eps_vir.reshape(1, v))

    return jax.shard_map(
        per_device,
        mesh=mesh,
        in_specs=(P(("frag", "dev")), P("frag"), P("frag"), P("frag"), P("frag")),
        out_specs=P("frag", "dev"),
        check_vma=False,
    )
```
